256 devices in a mesh: groups: 4 (over y, x), asset: 64 (over z, core).
Axes of the slice: x: 2, y: 2, z: 32, core: 2. Of those that a mesh axis runs over, the one named last changes fastest.
The devices are a block of a 4x8x32 slice.
Arguments:
- scen_draws: bfloat16 [16384, 256], P(('groups', 'asset')), parts along dimension 0, may hold values from -4 to 4
- factor_mix: bfloat16 [256, 256], replicated, may hold values from -0.375 to 0.375
- loadings: bfloat16 [262144, 256], P(('groups', 'asset')), parts along dimension 0, may hold values from -0.375 to 0.375
- convexity: float32 [262144], P(('groups', 'asset')), parts along dimension 0, may hold values from -0.6 to 0.6
- holdings: float32 [262144], P(('groups', 'asset')), parts along dimension 0, may hold values from -0.110485435 to 0.110485435
- desk_map: int32 [262144], P(('groups', 'asset')), parts along dimension 0, may hold values from 0 to 127
- ranks: int32 [16384], P('groups'), parts along dimension 0, may hold values from 0 to 4095, each once
- desk_prices: float32 [512], P('groups'), parts along dimension 0, may hold values from -5 to 5
Outputs:
- allocation: float32 [512], P('groups'), parts along dimension 0
- grad_loadings: float32 [262144, 256], P(('groups', 'asset')), parts along dimension 0
- grad_convexity: float32 [262144], P(('groups', 'asset')), parts along dimension 0
The draws below stay inside these ranges and needn't reach their ends.
There are 4 independent parts, one for each index of `groups`. The reference program is written for one: setup_inputs(seed, part) draws one part's arguments, and reference() takes and returns one part's arrays. A program takes and returns all parts, laid end to end along the dimension named above; an argument that names none is the same for every part. Nothing has to cross between parts.
All inputs are finite; a program needn't handle non-finite values.
Results may differ from the reference program's by a relative error of at most 0.0029.
Values may be sent and summed in bfloat16 or wider, within the bound.
No kernel may reach another device: no remote copies, remote signals or barrier semaphores. Data moves between devices by JAX's collectives and lax.ppermute only.
A program may use at most 64 MiB of HBM per device.

```python
import math
import jax
import jax.numpy as jnp
from jax import lax

F = 256
DESKS = 128
SCEN = 4096
ASSETS = 65536
BAND = 32
CENTER = 166


def draw_scen_draws(key, part):
    position = jnp.arange(SCEN, dtype=jnp.float32) / SCEN
    base = jax.random.normal(key, (SCEN, F), jnp.float32)
    growth = jnp.exp((position - 0.5) * math.log(3.0))
    return jnp.clip(base * growth[:, None], -4.0, 4.0).astype(jnp.bfloat16)


def draw_holdings(key, part):
    position = jnp.arange(ASSETS, dtype=jnp.float32) / ASSETS
    base = jax.random.normal(key, (ASSETS,), jnp.float32)
    growth = jnp.exp((position - 0.5) * math.log(3.0))
    return jnp.clip(base * growth, -2.5, 2.5) / math.sqrt(ASSETS // DESKS)


def place_ends(entries, stream_key, low, top_value):
    extent = entries.shape
    index_at = [jax.random.randint(jax.random.fold_in(stream_key, axis), (), 0, extent[axis]) for axis in range(len(extent))]
    entries = entries.at[tuple(index_at)].set(low)
    longest = extent.index(max(extent))
    index_at[longest] = (index_at[longest] + 1) % extent[longest]
    return entries.at[tuple(index_at)].set(top_value)


def steps_of(rng, dims, cuts, smallest, largest):
    def one(dim, parts):
        heights = jax.random.uniform(jax.random.fold_in(jax.random.fold_in(rng, 6), dim), (parts,), jnp.float32, smallest / len(cuts), largest / len(cuts))
        return jnp.repeat(jnp.exp(heights), dims[dim] // parts).reshape((-1,) + (1,) * (len(dims) - dim - 1))

    factor_of = one(*cuts[0])
    for cut in cuts[1:]:
        factor_of = factor_of * one(*cut)
    return factor_of


def normal_values(key, shape, deviation, reach, pieces=(), kind=jnp.bfloat16):
    array = jax.random.normal(key, shape, jnp.float32) * deviation
    if len(pieces) > 0:
        array = steps_of(key, shape, pieces, -0.22, 0.18) * array
    return jnp.clip(array, min=-reach, max=reach).astype(kind)


def setup_inputs(seed: int = 0, part: int = 0) -> dict:
    seeds = jax.random.split(jax.random.key(seed), 9)
    part_splits = jax.random.split(jax.random.fold_in(seeds[8], part), 9)
    scen_draws = draw_scen_draws(jax.random.fold_in(jax.random.fold_in(seeds[8], part), 71), part)
    factor_mix = normal_values(seeds[1], (F, F), F ** -0.5, 0.375)
    loadings = normal_values(part_splits[2], (ASSETS, F), F ** -0.5, 0.375, ((0, 64),))
    convexity = jnp.clip(jax.random.uniform(part_splits[3], (ASSETS,), jnp.float32, -0.6, 0.6) * steps_of(part_splits[3], (ASSETS,), ((0, 64),), -0.4, 0.0), -0.6, 0.6)
    holdings = draw_holdings(jax.random.fold_in(jax.random.fold_in(seeds[8], part), 71), part)
    desk_map = place_ends(jax.random.randint(part_splits[5], (ASSETS,), 0, DESKS), jax.random.fold_in(part_splits[5], 1), 0, DESKS - 1).astype(jnp.int32)
    ranks = jax.random.permutation(part_splits[6], SCEN).astype(jnp.int32)
    desk_prices = normal_values(part_splits[7], (DESKS,), 1.0, 5.0, (), jnp.float32)
    return dict(scen_draws=scen_draws, factor_mix=factor_mix, loadings=loadings, convexity=convexity, holdings=holdings, desk_map=desk_map, ranks=ranks, desk_prices=desk_prices)


def smooth_bend(value):
    return jnp.logaddexp(value, -value) - math.log(2.0)

def rank_kernel(ranks, scenarios):
    centre = jnp.float32(CENTER)
    spread = jnp.float32(BAND)
    offsets = (ranks.astype(jnp.float32) - centre) / spread
    every = (jnp.arange(scenarios, dtype=jnp.float32) - centre) / spread
    return jnp.exp(-0.5 * offsets * offsets) / jnp.sum(jnp.exp(-0.5 * every * every))

def cotangent_of(weights, weight_total, slopes, smoothing, kernel, grad_quant, grad_band, centred, prices, scenarios):
    grad_loss = slopes / smoothing + kernel * grad_quant + grad_band * 0.09 * centred / (scenarios * smoothing)
    return (scenarios * (-weights[:, None] * prices[None, :] / weight_total - grad_loss[:, None])).astype(jnp.bfloat16)

def tail_terms(desk_pnl, ranks, prices):
    scenarios = desk_pnl.shape[0]
    losses = -lax.optimization_barrier(jnp.sum(desk_pnl, axis=1))
    kernel = rank_kernel(ranks, scenarios)
    quantile = jnp.sum(kernel * losses)
    average = jnp.mean(losses)
    centred = losses - average
    smoothing = 0.3 * jnp.sqrt(jnp.mean(centred * centred) + 1e-06)
    scores = (losses - quantile) / smoothing
    weights = jax.nn.sigmoid(scores)
    weight_total = jnp.sum(weights)
    valued = lax.optimization_barrier(jnp.sum(desk_pnl * prices[None, :], axis=1))
    objective = -jnp.sum(weights * valued) / weight_total
    allocation = -lax.optimization_barrier(jnp.sum(weights[:, None] * desk_pnl, axis=0)) / weight_total
    slopes = (-valued - objective) / weight_total * weights * (1.0 - weights)
    grad_quant = -jnp.sum(slopes) / smoothing
    grad_band = -jnp.sum(slopes * scores) / smoothing
    cotangent = cotangent_of(weights, weight_total, slopes, smoothing, kernel, grad_quant, grad_band, centred, prices, scenarios)
    return (cotangent, allocation)

def exposure_of(shock_rows, loadings):
    return lax.dot_general(shock_rows, loadings, (((1,), (1,)), ((), ())), preferred_element_type=jnp.float32)

def reference(scen_draws, factor_mix, loadings, convexity, holdings, desk_map, ranks, desk_prices):
    shocks = jnp.dot(scen_draws, factor_mix, preferred_element_type=jnp.float32).astype(jnp.bfloat16)
    block_rows = math.gcd(SCEN, 256)
    shock_blocks = shocks.reshape((-1, block_rows, F))

    def forward(shock_block):
        exposure = exposure_of(shock_block, loadings)
        held = (holdings * (exposure + convexity * smooth_bend(exposure))).astype(jnp.bfloat16)
        summed = jax.ops.segment_sum(held.astype(jnp.float32).T, desk_map, num_segments=DESKS)
        return summed.T
    desk_pnl = lax.map(forward, shock_blocks).reshape((SCEN, DESKS))
    cotangent, allocation = tail_terms(desk_pnl, ranks, desk_prices)
    cot_blocks = cotangent.reshape((-1, block_rows, DESKS))

    def backward(state, inputs):
        shock_block, cot_block = inputs
        exposure = exposure_of(shock_block, loadings)
        held = holdings * cot_block[:, desk_map].astype(jnp.float32)
        grad_exposure = (held * (1.0 + convexity * jnp.tanh(exposure))).astype(jnp.bfloat16)
        grad_load = state[0] + lax.dot_general(grad_exposure, shock_block, (((0,), (0,)), ((), ())), preferred_element_type=jnp.float32)
        grad_conv = state[1] + lax.optimization_barrier(jnp.sum(held * smooth_bend(exposure), axis=0))
        return ((grad_load, grad_conv), None)
    initial = (jnp.zeros((ASSETS, F), jnp.float32), jnp.zeros((ASSETS,), jnp.float32))
    final, ignored = lax.scan(backward, initial, (shock_blocks, cot_blocks))
    grad_load, grad_conv = final
    squares = jnp.sum(grad_load * grad_load) + jnp.sum(grad_conv * grad_conv)
    factor = lax.rsqrt(squares / (ASSETS * (F + 1)) + 1e-06)
    return (allocation, grad_load * factor, grad_conv * factor)
```

```python
import math

import jax
import jax.numpy as jnp
import numpy as np
from jax import lax
from jax.experimental import pallas as pl
from jax.experimental.pallas import tpu as pltpu
from jax.sharding import Mesh
from jax.sharding import PartitionSpec as P

BAND = 32
CENTER = 166
FAR = 8
NEAR = 4
CLASSES = NEAR * 2
CHIPS = ("far", "near")
CLOSE = ("near", "core")
ASSET = ("far", "near", "core")
GROUPS_ASSET = ("groups", *ASSET)
LOG2 = math.log(2.0)
F32 = jnp.float32
BF16 = jnp.bfloat16
LANES = 128
TILE = 256
STEPS_Z = np.array([0, 0, 1, 3, 1, 3, 2, 2], np.int32)
OTHER = np.array([0, 1, 0, 0, 1, 1, 0, 1], np.int32)


def dot_of(a, b, dims, precision=None):
    return lax.dot_general(a, b, (dims, ((), ())), precision=precision, preferred_element_type=F32)


def forward_kernel(pieces, first, order_ref, *refs):
    shock_refs, refs = refs[:pieces], refs[pieces:]
    load_ref, conv_ref, hold_ref, desk_ref, price_ref = refs[:5]
    outs = refs[5:] if first else refs[10:]
    tanh_ref, bend_ref, pnl_ref, turned_ref, sums_ref, rows, table = outs
    step = pl.program_id(0)
    piece = shock_refs[0].shape[0]
    assets = load_ref.shape[0]
    desks = price_ref.shape[1]

    @pl.when(step == 0)
    def _():
        for i in range(pieces):
            rows[i * piece : (i + 1) * piece, :] = shock_refs[i][...]
        desk = lax.broadcasted_iota(jnp.int32, (desks, assets), 0)
        table[...] = jnp.where(desk == desk_ref[...], 1.0, 0.0).astype(BF16)

    size = tanh_ref.shape[0]
    shocks = rows[pl.ds(pl.multiple_of(step * size, size), size), :]
    turned_ref[...] = shocks.T
    pnl = jnp.zeros((size, desks), F32)
    for low in range(0, assets, TILE):
        part = slice(low, low + TILE)
        exposure = dot_of(shocks, load_ref[part, :], ((1,), (1,)))
        size_of = jnp.abs(exposure)
        bend = size_of + (jnp.log(1.0 + jnp.exp(-2.0 * size_of)) - LOG2)
        held = hold_ref[:, part] * (exposure + conv_ref[:, part] * bend)
        tanh_ref[:, part] = jnp.tanh(exposure).astype(BF16)
        bend_ref[:, part] = bend.astype(BF16)
        pnl = pnl + dot_of(held.astype(BF16), table[:, part], ((1,), (1,)))
    pnl_ref[...] = pnl
    row = lax.broadcasted_iota(jnp.int32, (8, desks), 0)
    weigh = jnp.where(row == 0, -1.0, jnp.where(row == 1, price_ref[...], 0.0))
    sums = dot_of(weigh, pnl, ((1,), (1,)), lax.Precision.HIGHEST)
    lines = size // LANES
    half = step % 2
    for part in range(2):
        for line in range(lines):
            sums_ref[0, pl.ds(part * 4 + half * lines + line, 1), :] = sums[
                part : part + 1, line * LANES : (line + 1) * LANES
            ]


def forward_call(shocks, place, order, loadings, convexity, holdings, desk_map, prices, held):
    pieces, piece, factors = len(shocks), *shocks[0].shape
    scenarios = piece * CLASSES
    assets, desks = loadings.shape[0], prices.shape[1]
    size = piece // 2
    first = held is None
    base = place * 2
    whole = lambda shape: pl.BlockSpec(shape, lambda i, o: (0, 0))
    out_shape = (
        jax.ShapeDtypeStruct((scenarios, assets), BF16),
        jax.ShapeDtypeStruct((scenarios, assets), BF16),
        jax.ShapeDtypeStruct((scenarios, desks), F32),
        jax.ShapeDtypeStruct((factors, scenarios), BF16),
        jax.ShapeDtypeStruct((CLASSES, 8, LANES), F32),
    )
    out_specs = (
        pl.BlockSpec((size, assets), lambda i, o: (base + i, 0)),
        pl.BlockSpec((size, assets), lambda i, o: (base + i, 0)),
        pl.BlockSpec((size, desks), lambda i, o: (base + i, 0)),
        pl.BlockSpec((factors, size), lambda i, o: (0, base + i)),
        pl.BlockSpec((1, 8, LANES), lambda i, o: (o[place + i // 2], 0, 0)),
    )
    in_specs = [whole((piece, factors))] * pieces + [
        whole((assets, factors)),
        whole((1, assets)),
        whole((1, assets)),
        whole((1, assets)),
        whole((1, desks)),
    ]
    operands = [*shocks, loadings, convexity, holdings, desk_map, prices]
    aliases = {}
    if not first:
        aliases = {1 + len(operands) + i: i for i in range(5)}
        in_specs += [pl.BlockSpec(memory_space=pl.ANY)] * 5
        operands += list(held)
    return pl.pallas_call(
        lambda *refs: forward_kernel(pieces, first, *refs),
        grid_spec=pltpu.PrefetchScalarGridSpec(
            num_scalar_prefetch=1,
            grid=(pieces * 2,),
            in_specs=in_specs,
            out_specs=out_specs,
            scratch_shapes=[
                pltpu.VMEM((pieces * piece, factors), BF16),
                pltpu.VMEM((desks, assets), BF16),
            ],
        ),
        out_shape=out_shape,
        input_output_aliases=aliases,
        compiler_params=pltpu.CompilerParams(dimension_semantics=("arbitrary",)),
        cost_estimate=pl.CostEstimate(
            flops=2 * pieces * piece * assets * (factors + desks),
            bytes_accessed=pieces * piece * assets * 4,
            transcendentals=3 * pieces * piece * assets,
        ),
        name=f"forward_{place}",
    )(order, *operands)


def total(x):
    x = jnp.sum(x, axis=0, keepdims=True)
    x = jnp.sum(x, axis=1, keepdims=True)
    return jnp.sum(x, axis=2, keepdims=True)


def tail_of(losses, valued, ranks):
    scenarios = losses.size
    place = (
        lax.broadcasted_iota(jnp.int32, losses.shape, 0) * (losses.shape[1] * LANES)
        + lax.broadcasted_iota(jnp.int32, losses.shape, 1) * LANES
        + lax.broadcasted_iota(jnp.int32, losses.shape, 2)
    )
    offsets = (ranks.astype(F32) - CENTER) / BAND
    every = (place.astype(F32) - CENTER) / BAND
    kernel = jnp.exp(-0.5 * offsets * offsets) / total(jnp.exp(-0.5 * every * every))
    quantile = total(kernel * losses)
    average = total(losses) / scenarios
    centred = losses - average
    smoothing = 0.3 * jnp.sqrt(total(centred * centred) / scenarios + 1e-06)
    scores = (losses - quantile) / smoothing
    weights = 1.0 / (1.0 + jnp.exp(-scores))
    weight_total = total(weights)
    objective = -total(weights * valued) / weight_total
    slopes = (-valued - objective) / weight_total * weights * (1.0 - weights)
    grad_quant = -total(slopes) / smoothing
    grad_band = -total(slopes * scores) / smoothing
    grad_loss = (
        slopes / smoothing
        + kernel * grad_quant
        + grad_band * 0.09 * centred / (scenarios * smoothing)
    )
    return (-scenarios * weights / weight_total, -scenarios * grad_loss)


def backward_kernel(order_ref, *refs):
    sums_ref, ranks_ref, tanh_ref, bend_ref, pnl_ref, turned_ref = refs[:6]
    conv_ref, hold_ref, desk_ref, price_ref = refs[6:10]
    raw_ref, line_ref, last_ref, scaled, lines, wide, line_sums, both = refs[10:]
    step = pl.program_id(0)
    factors, scenarios = turned_ref.shape
    desks = price_ref.shape[0]
    piece = scenarios // CLASSES
    cuts = piece // LANES

    @pl.when(step == 0)
    def _():
        w, g = tail_of(sums_ref[:, 0:cuts, :], sums_ref[:, cuts : 2 * cuts, :], ranks_ref[...])
        both[:, 0:cuts, :] = w
        both[:, cuts : 2 * cuts, :] = g
        alloc = jnp.zeros((8, desks), F32)
        sum_w = jnp.zeros((factors, LANES), F32)
        sum_g = jnp.zeros((factors, LANES), F32)
        for i in range(CLASSES):
            kind = order_ref[i]
            rows_w, rows_g = [], []
            for j in range(cuts):
                span = slice(i * piece + j * LANES, i * piece + (j + 1) * LANES)
                turned = turned_ref[:, span].astype(F32)
                row_w = both[kind, j : j + 1, :]
                row_g = both[kind, cuts + j : cuts + j + 1, :]
                by_w = turned * row_w
                by_g = turned * row_g
                sum_w = sum_w + by_w
                sum_g = sum_g + by_g
                scaled[0:factors, span] = by_w.astype(BF16)
                scaled[factors : 2 * factors, span] = by_g.astype(BF16)
                rows_w.append(row_w)
                rows_g.append(row_g)
            row_w = jnp.concatenate(rows_w, axis=1)
            row_g = jnp.concatenate(rows_g, axis=1)
            wide_w = jnp.broadcast_to(row_w, (8, piece))
            wide_g = jnp.broadcast_to(row_g, (8, piece))
            place = lax.broadcasted_iota(jnp.int32, (8, piece), 0)
            value = jnp.where(place < 2, wide_w, wide_g)
            high = value.astype(BF16).astype(F32)
            lines[:, i * piece : (i + 1) * piece] = jnp.where(place % 2 == 0, high, value - high).astype(
                BF16
            )
            alloc = alloc + dot_of(
                wide_w, pnl_ref[i * piece : (i + 1) * piece, :], ((1,), (0,)), lax.Precision.HIGHEST
            )
        wide[:, 0:1] = jnp.sum(sum_w, axis=1, keepdims=True)
        wide[:, 1:2] = jnp.sum(sum_g, axis=1, keepdims=True)
        last_ref[:, 0:desks] = alloc[0:1, :] / scenarios
        last_ref[:, desks : 2 * desks] = jnp.zeros((1, desks), F32)

    held = hold_ref[...]
    desk = lax.broadcasted_iota(jnp.int32, (desks, held.shape[1]), 0)
    prices = jnp.sum(jnp.where(desk == desk_ref[...], price_ref[...], 0.0), axis=0, keepdims=True)
    curved = dot_of(scaled[...], tanh_ref[...], ((1,), (0,)))
    bent = dot_of(lines[...], bend_ref[...], ((1,), (0,)))
    line = held * (prices * (bent[0:1, :] + bent[1:2, :]) + (bent[2:3, :] + bent[3:4, :]))
    raw = (conv_ref[...] * held) * (prices * curved[0:factors, :] + curved[factors:, :]) + held * (
        prices * wide[:, 0:1] + wide[:, 1:2]
    )
    raw_ref[...] = raw.T
    line_ref[...] = line
    squares = jnp.sum(raw * raw, axis=0, keepdims=True) + line * line
    for low in range(0, squares.shape[1], desks):
        last_ref[:, desks : 2 * desks] += squares[:, low : low + desks]


def backward_call(order, sums, ranks, held, convexity, holdings, desk_map, prices):
    tanh, bend, pnl, turned = held
    scenarios, assets = tanh.shape
    factors, desks = turned.shape[0], pnl.shape[1]
    whole = lambda *shape: pl.BlockSpec(shape, lambda i, o: (0,) * len(shape))
    line = pl.BlockSpec((1, TILE), lambda i, o: (0, i))
    column = pl.BlockSpec((scenarios, TILE), lambda i, o: (0, i))
    return pl.pallas_call(
        backward_kernel,
        grid_spec=pltpu.PrefetchScalarGridSpec(
            num_scalar_prefetch=1,
            grid=(assets // TILE,),
            in_specs=[
                whole(*sums.shape),
                whole(*ranks.shape),
                column,
                column,
                whole(scenarios, desks),
                whole(factors, scenarios),
                line,
                line,
                line,
                whole(desks, 1),
            ],
            out_specs=(
                pl.BlockSpec((TILE, factors), lambda i, o: (i, 0)),
                line,
                whole(1, 2 * desks),
            ),
            scratch_shapes=[
                pltpu.VMEM((2 * factors, scenarios), BF16),
                pltpu.VMEM((8, scenarios), BF16),
                pltpu.VMEM((factors, 2), F32),
                pltpu.VMEM((8, LANES), F32),
                pltpu.VMEM(sums.shape, F32),
            ],
        ),
        out_shape=(
            jax.ShapeDtypeStruct((assets, factors), F32),
            jax.ShapeDtypeStruct((1, assets), F32),
            jax.ShapeDtypeStruct((1, 2 * desks), F32),
        ),
        compiler_params=pltpu.CompilerParams(dimension_semantics=("arbitrary",)),
        cost_estimate=pl.CostEstimate(
            flops=4 * scenarios * assets * factors,
            bytes_accessed=scenarios * assets * 4,
            transcendentals=0,
        ),
        name="backward",
    )(order, sums, ranks, tanh, bend, pnl, turned, convexity, holdings, desk_map, prices)


def scale_kernel(entries, parts_ref, raw_ref, line_ref, alloc_ref, grad_ref, conv_ref):
    whole = jnp.sum(parts_ref[...], axis=0)
    desks = alloc_ref.shape[1]
    alloc_ref[...] = whole[:, 0:desks]
    squares = jnp.sum(whole[:, desks:], axis=1, keepdims=True)
    factor = lax.rsqrt(squares / entries + 1e-06)
    grad_ref[...] = raw_ref[...] * factor
    conv_ref[...] = line_ref[...] * factor


def scale_call(parts, raw, line, entries):
    desks = parts.shape[2] // 2
    return pl.pallas_call(
        lambda *refs: scale_kernel(entries, *refs),
        out_shape=(
            jax.ShapeDtypeStruct((1, desks), F32),
            jax.ShapeDtypeStruct(raw.shape, F32),
            jax.ShapeDtypeStruct(line.shape, F32),
        ),
        name="scale",
    )(parts, raw, line)


def for_each(x, axis):
    return lax.all_to_all(
        jnp.broadcast_to(x, (lax.axis_size(axis), *x.shape)), axis, 0, 0, tiled=True
    )


def shards(scen_draws, factor_mix, loadings, convexity, holdings, desk_map, ranks, desk_prices):
    chips = FAR * NEAR
    near, core = lax.axis_index("near"), lax.axis_index("core")
    order = ((near + STEPS_Z) % NEAR) * 2 + (core + OTHER) % 2
    up = [(i, (i - 1) % chips) for i in range(chips)]
    down = [(i, (i + 1) % chips) for i in range(chips)]
    swap = lambda x: lax.ppermute(x, "core", [(0, 1), (1, 0)])
    from_up = lambda x: lax.ppermute(x, CHIPS, up)
    from_down = lambda x: lax.ppermute(x, CHIPS, down)

    local = jnp.dot(scen_draws, factor_mix, preferred_element_type=F32).astype(BF16)
    own = for_each(local, "far").reshape(-1, local.shape[1])
    half = own.shape[0] // 2
    lines = [x.reshape(1, -1) for x in (convexity, holdings, desk_map)]
    forward = lambda shocks, place, held: forward_call(
        shocks, place, order, loadings, *lines, desk_prices.reshape(1, -1), held
    )
    next_up, next_down = from_up(own), from_down(own)
    own_other = swap(own)
    held = forward([own, own_other], 0, None)
    next_up, next_down, held = lax.optimization_barrier((next_up, next_down, held))
    two_up = from_up(next_up[:half])
    two_down = from_down(next_down[half:])
    up_other, down_other = swap(next_up), swap(next_down)
    held = forward([next_up, next_down, up_other, down_other], 2, held)
    two_up, two_down, held = lax.optimization_barrier((two_up, two_down, held))
    two = jnp.concatenate([two_up, two_down])
    held = forward([two, swap(two)], 6, held)

    mine = jnp.sum(lax.all_to_all(held[4], CLOSE, 0, 0, tiled=True), axis=0)
    mine = jnp.sum(for_each(mine, "far"), axis=0)
    sums = for_each(mine, CLOSE)
    placed = ranks.reshape(FAR, CLASSES, -1).transpose(1, 0, 2).reshape(CLASSES, -1, LANES)
    raw, line, last = backward_call(
        order, sums, placed, held[:4], *lines, desk_prices.reshape(-1, 1)
    )
    entries = loadings.shape[0] * lax.axis_size(ASSET) * (loadings.shape[1] + 1)
    alloc, grad, conv = scale_call(for_each(last, ASSET), raw, line, entries)
    return (alloc.reshape(-1), grad, conv.reshape(-1))


def solution(mesh):
    torus = Mesh(
        mesh.devices.reshape(mesh.shape["groups"], FAR, NEAR, 2), ("groups", *ASSET)
    )
    return jax.shard_map(
        shards,
        mesh=torus,
        in_specs=(
            P(GROUPS_ASSET, None),
            P(),
            P(GROUPS_ASSET, None),
            P(GROUPS_ASSET),
            P(GROUPS_ASSET),
            P(GROUPS_ASSET),
            P("groups"),
            P("groups"),
        ),
        out_specs=(P("groups"), P(GROUPS_ASSET, None), P(GROUPS_ASSET)),
        check_vma=False,
    )
```

```python
import math

import jax
import jax.numpy as jnp
import numpy as np
from jax import lax
from jax.experimental import pallas as pl
from jax.experimental.pallas import tpu as pltpu
from jax.sharding import Mesh
from jax.sharding import PartitionSpec as P

BAND = 32
CENTER = 166
FAR = 8
NEAR = 4
CLASSES = NEAR * 2
CHIPS = ("far", "near")
CLOSE = ("near", "core")
ASSET = ("far", "near", "core")
GROUPS_ASSET = ("groups", *ASSET)
LOG2 = math.log(2.0)
F32 = jnp.float32
BF16 = jnp.bfloat16
LANES = 128
TILE = 256
FORWARD_VMEM = 16 << 20
BACKWARD_VMEM = 20 << 20
SCALE_VMEM = 8 << 20
STEPS_Z = np.array([0, 0, 1, 3, 1, 3, 2, 2], np.int32)
OTHER = np.array([0, 1, 0, 0, 1, 1, 0, 1], np.int32)


def dot_of(a, b, dims, precision=None):
    return lax.dot_general(a, b, (dims, ((), ())), precision=precision, preferred_element_type=F32)


def forward_kernel(pieces, first, order_ref, *refs):
    shock_refs, refs = refs[:pieces], refs[pieces:]
    load_ref, conv_ref, hold_ref, desk_ref, price_ref = refs[:5]
    outs = refs[5:] if first else refs[10:]
    tanh_ref, bend_ref, pnl_ref, turned_ref, sums_ref, rows, table = outs
    step = pl.program_id(0)
    piece = shock_refs[0].shape[0]
    assets = load_ref.shape[0]
    desks = price_ref.shape[1]

    @pl.when(step == 0)
    def _():
        for i in range(pieces):
            rows[i * piece : (i + 1) * piece, :] = shock_refs[i][...]
        desk = lax.broadcasted_iota(jnp.int32, (desks, assets), 0)
        table[...] = jnp.where(desk == desk_ref[...], 1.0, 0.0).astype(BF16)

    size = tanh_ref.shape[0]
    shocks = rows[pl.ds(pl.multiple_of(step * size, size), size), :]
    turned_ref[...] = shocks.T
    pnl = jnp.zeros((size, desks), F32)
    for low in range(0, assets, TILE):
        part = slice(low, low + TILE)
        exposure = dot_of(shocks, load_ref[part, :], ((1,), (1,)))
        size_of = jnp.abs(exposure)
        bend = size_of + (jnp.log(1.0 + jnp.exp(-2.0 * size_of)) - LOG2)
        held = hold_ref[:, part] * (exposure + conv_ref[:, part] * bend)
        tanh_ref[:, part] = jnp.tanh(exposure).astype(BF16)
        bend_ref[:, part] = bend.astype(BF16)
        pnl = pnl + dot_of(held.astype(BF16), table[:, part], ((1,), (1,)))
    pnl_ref[...] = pnl
    row = lax.broadcasted_iota(jnp.int32, (8, desks), 0)
    weigh = jnp.where(row == 0, -1.0, jnp.where(row == 1, price_ref[...], 0.0))
    sums = dot_of(weigh, pnl, ((1,), (1,)), lax.Precision.HIGHEST)
    lines = size // LANES
    for part in range(2):
        for line in range(lines):
            sums_ref[0, part * lines + line : part * lines + line + 1, :] = sums[
                part : part + 1, line * LANES : (line + 1) * LANES
            ]


def forward_call(shocks, place, order, loadings, convexity, holdings, desk_map, prices, held):
    pieces, piece, factors = len(shocks), *shocks[0].shape
    scenarios = piece * CLASSES
    assets, desks = loadings.shape[0], prices.shape[1]
    size = piece
    first = held is None
    base = place
    whole = lambda shape: pl.BlockSpec(shape, lambda i, o: (0, 0))
    out_shape = (
        jax.ShapeDtypeStruct((scenarios, assets), BF16),
        jax.ShapeDtypeStruct((scenarios, assets), BF16),
        jax.ShapeDtypeStruct((scenarios, desks), F32),
        jax.ShapeDtypeStruct((factors, scenarios), BF16),
        jax.ShapeDtypeStruct((CLASSES, 8, LANES), F32),
    )
    out_specs = (
        pl.BlockSpec((size, assets), lambda i, o: (base + i, 0)),
        pl.BlockSpec((size, assets), lambda i, o: (base + i, 0)),
        pl.BlockSpec((size, desks), lambda i, o: (base + i, 0)),
        pl.BlockSpec((factors, size), lambda i, o: (0, base + i)),
        pl.BlockSpec((1, 8, LANES), lambda i, o: (o[place + i], 0, 0)),
    )
    in_specs = [whole((piece, factors))] * pieces + [
        whole((assets, factors)),
        whole((1, assets)),
        whole((1, assets)),
        whole((1, assets)),
        whole((1, desks)),
    ]
    operands = [*shocks, loadings, convexity, holdings, desk_map, prices]
    aliases = {}
    if not first:
        aliases = {1 + len(operands) + i: i for i in range(5)}
        in_specs += [pl.BlockSpec(memory_space=pl.ANY)] * 5
        operands += list(held)
    return pl.pallas_call(
        lambda *refs: forward_kernel(pieces, first, *refs),
        grid_spec=pltpu.PrefetchScalarGridSpec(
            num_scalar_prefetch=1,
            grid=(pieces,),
            in_specs=in_specs,
            out_specs=out_specs,
            scratch_shapes=[
                pltpu.VMEM((pieces * piece, factors), BF16),
                pltpu.VMEM((desks, assets), BF16),
            ],
        ),
        out_shape=out_shape,
        input_output_aliases=aliases,
        compiler_params=pltpu.CompilerParams(
            dimension_semantics=("arbitrary",), vmem_limit_bytes=FORWARD_VMEM
        ),
        cost_estimate=pl.CostEstimate(
            flops=2 * pieces * piece * assets * (factors + desks),
            bytes_accessed=pieces * piece * assets * 4,
            transcendentals=3 * pieces * piece * assets,
        ),
        name=f"forward_{place}",
    )(order, *operands)


def total(x):
    x = jnp.sum(x, axis=0, keepdims=True)
    x = jnp.sum(x, axis=1, keepdims=True)
    return jnp.sum(x, axis=2, keepdims=True)


def tail_of(losses, valued, ranks):
    scenarios = losses.size
    place = (
        lax.broadcasted_iota(jnp.int32, losses.shape, 0) * (losses.shape[1] * LANES)
        + lax.broadcasted_iota(jnp.int32, losses.shape, 1) * LANES
        + lax.broadcasted_iota(jnp.int32, losses.shape, 2)
    )
    offsets = (ranks - CENTER) / BAND
    every = (place.astype(F32) - CENTER) / BAND
    kernel = jnp.exp(-0.5 * offsets * offsets) / total(jnp.exp(-0.5 * every * every))
    quantile = total(kernel * losses)
    average = total(losses) / scenarios
    centred = losses - average
    smoothing = 0.3 * jnp.sqrt(total(centred * centred) / scenarios + 1e-06)
    scores = (losses - quantile) / smoothing
    weights = 1.0 / (1.0 + jnp.exp(-scores))
    weight_total = total(weights)
    objective = -total(weights * valued) / weight_total
    slopes = (-valued - objective) / weight_total * weights * (1.0 - weights)
    grad_quant = -total(slopes) / smoothing
    grad_band = -total(slopes * scores) / smoothing
    grad_loss = (
        slopes / smoothing
        + kernel * grad_quant
        + grad_band * 0.09 * centred / (scenarios * smoothing)
    )
    return (-scenarios * weights / weight_total, -scenarios * grad_loss)


def backward_kernel(order_ref, *refs):
    sums_ref, ranks_ref, tanh_ref, bend_ref, pnl_ref, turned_ref = refs[:6]
    conv_ref, hold_ref, desk_ref, price_ref = refs[6:10]
    raw_ref, line_ref, last_ref, scaled, lines, wide, placed, both = refs[10:]
    step = pl.program_id(0)
    factors, scenarios = turned_ref.shape
    desks = price_ref.shape[1]
    piece = scenarios // CLASSES
    cuts = piece // LANES

    @pl.when(step == 0)
    def _():
        low = lax.broadcasted_iota(jnp.int32, (1, LANES), 1) < LANES // 2
        for q in range(cuts):
            for j in range(cuts):
                here = ranks_ref[2 * j * cuts + q : 2 * j * cuts + q + 1, :].astype(F32)
                there = ranks_ref[(2 * j + 1) * cuts + q : (2 * j + 1) * cuts + q + 1, :].astype(F32)
                placed[2 * q, j : j + 1, :] = jnp.where(low, here, pltpu.roll(there, LANES // 2, 1))
                placed[2 * q + 1, j : j + 1, :] = jnp.where(
                    low, pltpu.roll(here, LANES // 2, 1), there
                )
        w, g = tail_of(sums_ref[:, 0:cuts, :], sums_ref[:, cuts : 2 * cuts, :], placed[...])
        both[:, 0:cuts, :] = w
        both[:, cuts : 2 * cuts, :] = g
        alloc = jnp.zeros((8, desks), F32)
        sum_w = jnp.zeros((factors, LANES), F32)
        sum_g = jnp.zeros((factors, LANES), F32)
        for i in range(CLASSES):
            kind = order_ref[i]
            rows_w, rows_g = [], []
            for j in range(cuts):
                span = slice(i * piece + j * LANES, i * piece + (j + 1) * LANES)
                turned = turned_ref[:, span].astype(F32)
                row_w = both[kind, j : j + 1, :]
                row_g = both[kind, cuts + j : cuts + j + 1, :]
                by_w = turned * row_w
                by_g = turned * row_g
                sum_w = sum_w + by_w
                sum_g = sum_g + by_g
                scaled[0:factors, span] = by_w.astype(BF16)
                scaled[factors : 2 * factors, span] = by_g.astype(BF16)
                rows_w.append(row_w)
                rows_g.append(row_g)
            row_w = jnp.concatenate(rows_w, axis=1)
            row_g = jnp.concatenate(rows_g, axis=1)
            wide_w = jnp.broadcast_to(row_w, (8, piece))
            wide_g = jnp.broadcast_to(row_g, (8, piece))
            place = lax.broadcasted_iota(jnp.int32, (8, piece), 0)
            value = jnp.where(place < 2, wide_w, wide_g)
            high = value.astype(BF16).astype(F32)
            lines[:, i * piece : (i + 1) * piece] = jnp.where(place % 2 == 0, high, value - high).astype(
                BF16
            )
            alloc = alloc + dot_of(
                wide_w, pnl_ref[i * piece : (i + 1) * piece, :], ((1,), (0,)), lax.Precision.HIGHEST
            )
        wide[:, 0:1] = jnp.sum(sum_w, axis=1, keepdims=True)
        wide[:, 1:2] = jnp.sum(sum_g, axis=1, keepdims=True)
        last_ref[:, 0:desks] = alloc[0:1, :] / scenarios
        last_ref[:, desks : 2 * desks] = jnp.zeros((1, desks), F32)

    held = hold_ref[...]
    desk = lax.broadcasted_iota(jnp.int32, (desks, held.shape[1]), 0)
    own = jnp.where(desk == desk_ref[...], 1.0, 0.0)
    wide_price = jnp.broadcast_to(price_ref[...], (8, desks))
    prices = dot_of(wide_price, own, ((1,), (0,)), lax.Precision.HIGHEST)[0:1, :]
    part = pl.ds(pl.multiple_of(step * TILE, TILE), TILE)
    curved = dot_of(scaled[...], tanh_ref[:, part], ((1,), (0,)))
    bent = dot_of(lines[...], bend_ref[:, part], ((1,), (0,)))
    line = held * (prices * (bent[0:1, :] + bent[1:2, :]) + (bent[2:3, :] + bent[3:4, :]))
    raw = (conv_ref[...] * held) * (prices * curved[0:factors, :] + curved[factors:, :]) + held * (
        prices * wide[:, 0:1] + wide[:, 1:2]
    )
    raw_ref[...] = raw.T
    line_ref[...] = line
    squares = jnp.sum(raw * raw, axis=0, keepdims=True) + line * line
    for low in range(0, squares.shape[1], desks):
        last_ref[:, desks : 2 * desks] += squares[:, low : low + desks]


def backward_call(order, sums, ranks, held, convexity, holdings, desk_map, prices):
    tanh, bend, pnl, turned = held
    scenarios, assets = tanh.shape
    factors, desks = turned.shape[0], pnl.shape[1]
    whole = lambda *shape: pl.BlockSpec(shape, lambda i, o: (0,) * len(shape))
    line = pl.BlockSpec((1, TILE), lambda i, o: (0, i))
    return pl.pallas_call(
        backward_kernel,
        grid_spec=pltpu.PrefetchScalarGridSpec(
            num_scalar_prefetch=1,
            grid=(assets // TILE,),
            in_specs=[
                whole(*sums.shape),
                whole(*ranks.shape),
                whole(scenarios, assets),
                whole(scenarios, assets),
                whole(scenarios, desks),
                whole(factors, scenarios),
                line,
                line,
                line,
                whole(1, desks),
            ],
            out_specs=(
                pl.BlockSpec((TILE, factors), lambda i, o: (i, 0)),
                line,
                whole(1, 2 * desks),
            ),
            scratch_shapes=[
                pltpu.VMEM((2 * factors, scenarios), BF16),
                pltpu.VMEM((8, scenarios), BF16),
                pltpu.VMEM((factors, 2), F32),
                pltpu.VMEM((CLASSES, sums.shape[1] // 2, LANES), F32),
                pltpu.VMEM(sums.shape, F32),
            ],
        ),
        out_shape=(
            jax.ShapeDtypeStruct((assets, factors), F32),
            jax.ShapeDtypeStruct((1, assets), F32),
            jax.ShapeDtypeStruct((1, 2 * desks), F32),
        ),
        compiler_params=pltpu.CompilerParams(
            dimension_semantics=("arbitrary",), vmem_limit_bytes=BACKWARD_VMEM
        ),
        cost_estimate=pl.CostEstimate(
            flops=4 * scenarios * assets * factors,
            bytes_accessed=scenarios * assets * 4,
            transcendentals=0,
        ),
        name="backward",
    )(order, sums, ranks, tanh, bend, pnl, turned, convexity, holdings, desk_map, prices)


def scale_kernel(entries, parts_ref, raw_ref, line_ref, alloc_ref, grad_ref, conv_ref):
    whole = jnp.sum(parts_ref[...], axis=0)
    desks = alloc_ref.shape[1]
    alloc_ref[...] = whole[:, 0:desks]
    squares = jnp.sum(whole[:, desks:], axis=1, keepdims=True)
    factor = lax.rsqrt(squares / entries + 1e-06)
    grad_ref[...] = raw_ref[...] * factor
    conv_ref[...] = line_ref[...] * factor


def scale_call(parts, raw, line, entries):
    desks = parts.shape[2] // 2
    return pl.pallas_call(
        lambda *refs: scale_kernel(entries, *refs),
        out_shape=(
            jax.ShapeDtypeStruct((1, desks), F32),
            jax.ShapeDtypeStruct(raw.shape, F32),
            jax.ShapeDtypeStruct(line.shape, F32),
        ),
        compiler_params=pltpu.CompilerParams(vmem_limit_bytes=SCALE_VMEM),
        name="scale",
    )(parts, raw, line)


def summed_kernel(x_ref, out_ref):
    out_ref[...] = jnp.broadcast_to(jnp.sum(x_ref[...], axis=0, keepdims=True), out_ref.shape)


def summed_copies(x, copies):
    return pl.pallas_call(
        summed_kernel,
        out_shape=jax.ShapeDtypeStruct((copies, *x.shape[1:]), F32),
        compiler_params=pltpu.CompilerParams(vmem_limit_bytes=1 << 20),
        name="summed_copies",
    )(x)


def for_each(x, axis):
    return lax.all_to_all(
        jnp.broadcast_to(x, (lax.axis_size(axis), *x.shape)), axis, 0, 0, tiled=True
    )


def shards(scen_draws, factor_mix, loadings, convexity, holdings, desk_map, ranks, desk_prices):
    chips = FAR * NEAR
    near, core = lax.axis_index("near"), lax.axis_index("core")
    order = ((near + STEPS_Z) % NEAR) * 2 + (core + OTHER) % 2
    up = [(i, (i - 1) % chips) for i in range(chips)]
    down = [(i, (i + 1) % chips) for i in range(chips)]
    swap = lambda x: lax.ppermute(x, "core", [(0, 1), (1, 0)])
    from_up = lambda x: lax.ppermute(x, CHIPS, up)
    from_down = lambda x: lax.ppermute(x, CHIPS, down)

    local = jnp.dot(scen_draws, factor_mix, preferred_element_type=F32).astype(BF16)
    own = for_each(local, "far").reshape(-1, local.shape[1])
    half = own.shape[0] // 2
    lines = [x.reshape(1, -1) for x in (convexity, holdings, desk_map)]
    forward = lambda shocks, place, held: forward_call(
        shocks, place, order, loadings, *lines, desk_prices.reshape(1, -1), held
    )
    next_up, next_down = from_up(own), from_down(own)
    own_other = swap(own)
    held = forward([own, own_other], 0, None)
    next_up, next_down, held = lax.optimization_barrier((next_up, next_down, held))
    two_up = from_up(next_up[:half])
    two_down = from_down(next_down[half:])
    up_other, down_other = swap(next_up), swap(next_down)
    held = forward([next_up, next_down, up_other, down_other], 2, held)
    two_up, two_down, held = lax.optimization_barrier((two_up, two_down, held))
    two = jnp.concatenate([two_up, two_down])
    held = forward([two, swap(two)], 6, held)

    mine = summed_copies(lax.all_to_all(held[4], CLOSE, 0, 0, tiled=True), FAR)
    mine = summed_copies(lax.all_to_all(mine, "far", 0, 0, tiled=True), CLASSES)
    sums = lax.all_to_all(mine, CLOSE, 0, 0, tiled=True)
    placed = ranks.reshape(-1, LANES)
    raw, line, last = backward_call(
        order, sums, placed, held[:4], *lines, desk_prices.reshape(1, -1)
    )
    entries = loadings.shape[0] * lax.axis_size(ASSET) * (loadings.shape[1] + 1)
    alloc, grad, conv = scale_call(for_each(last, ASSET), raw, line, entries)
    return (alloc.reshape(-1), grad, conv.reshape(-1))


def solution(mesh):
    torus = Mesh(
        mesh.devices.reshape(mesh.shape["groups"], FAR, NEAR, 2), ("groups", *ASSET)
    )
    return jax.shard_map(
        shards,
        mesh=torus,
        in_specs=(
            P(GROUPS_ASSET, None),
            P(),
            P(GROUPS_ASSET, None),
            P(GROUPS_ASSET),
            P(GROUPS_ASSET),
            P(GROUPS_ASSET),
            P("groups"),
            P("groups"),
        ),
        out_specs=(P("groups"), P(GROUPS_ASSET, None), P(GROUPS_ASSET)),
        check_vma=False,
    )
```

```python
import math

import jax
import jax.numpy as jnp
import numpy as np
from jax import lax
from jax.experimental import pallas as pl
from jax.experimental.pallas import tpu as pltpu
from jax.sharding import Mesh
from jax.sharding import PartitionSpec as P

BAND = 32
CENTER = 166
FAR = 8
NEAR = 4
CLASSES = NEAR * 2
CHIPS = ("far", "near")
CLOSE = ("near", "core")
ASSET = ("far", "near", "core")
GROUPS_ASSET = ("groups", *ASSET)
LOG2 = math.log(2.0)
F32 = jnp.float32
BF16 = jnp.bfloat16
LANES = 128
TILE = 256
PREPARE_VMEM = 65_900_000
FORWARD_VMEM = 16 << 20
BACKWARD_VMEM = 20 << 20
SCALE_VMEM = 8 << 20
STEPS_Z = np.array([0, 0, 1, 3, 1, 3, 2, 2], np.int32)
OTHER = np.array([0, 1, 0, 0, 1, 1, 0, 1], np.int32)


def dot_of(a, b, dims, precision=None):
    return lax.dot_general(a, b, (dims, ((), ())), precision=precision, preferred_element_type=F32)


def prepare_kernel(*refs):
    given, refs = refs[:6], refs[6:]
    copies_ref, table_ref, asset_ref = refs[:3]
    draws, mix, conv, hold, desk, price, sems = refs[3:]
    moves = [
        pltpu.make_async_copy(source, target, sems.at[i])
        for i, (source, target) in enumerate(
            zip(given, (draws, mix, desk, price, conv, hold))
        )
    ]
    for move in moves:
        move.start()
    for move in moves[:2]:
        move.wait()
    local = dot_of(draws[...], mix[...], ((1,), (0,))).astype(BF16)
    copies_ref[...] = jnp.broadcast_to(local[None], copies_ref.shape)
    for move in moves[2:]:
        move.wait()
    desks, assets = table_ref.shape
    place = lax.broadcasted_iota(jnp.int32, (desks, assets), 0)
    own = jnp.where(place == desk[...], 1.0, 0.0)
    table_ref[...] = own.astype(BF16)
    wide = jnp.broadcast_to(price[...], (8, desks))
    asset_ref[0:1, :] = conv[...]
    asset_ref[1:2, :] = hold[...]
    asset_ref[2:3, :] = dot_of(wide, own, ((1,), (0,)), lax.Precision.HIGHEST)[0:1, :]
    asset_ref[3:4, 0:desks] = price[...]


def prepare_call(scen_draws, factor_mix, desk_map, prices, convexity, holdings):
    assets, desks = desk_map.shape[1], prices.shape[1]
    hbm = pl.BlockSpec(memory_space=pltpu.HBM)
    vmem = pl.BlockSpec(memory_space=pltpu.VMEM)
    row = pltpu.VMEM((1, assets), F32)
    return pl.pallas_call(
        prepare_kernel,
        in_specs=[hbm] * 6,
        out_specs=(vmem,) * 3,
        out_shape=(
            jax.ShapeDtypeStruct((FAR, *scen_draws.shape), BF16),
            jax.ShapeDtypeStruct((desks, assets), BF16),
            jax.ShapeDtypeStruct((8, assets), F32),
        ),
        scratch_shapes=[
            pltpu.VMEM(scen_draws.shape, BF16),
            pltpu.VMEM(factor_mix.shape, BF16),
            row,
            row,
            pltpu.VMEM((1, assets), jnp.int32),
            pltpu.VMEM((1, desks), F32),
            pltpu.SemaphoreType.DMA((6,)),
        ],
        compiler_params=pltpu.CompilerParams(vmem_limit_bytes=PREPARE_VMEM),
        name="prepare",
    )(scen_draws, factor_mix, desk_map, prices, convexity, holdings)


def forward_kernel(pieces, first, order_ref, *refs):
    shock_refs, refs = refs[:pieces], refs[pieces:]
    load_ref, table, asset_ref = refs[:3]
    outs = refs[3:] if first else refs[8:]
    tanh_ref, bend_ref, pnl_ref, turned_ref, sums_ref, rows = outs
    step = pl.program_id(0)
    piece = shock_refs[0].shape[0]
    desks, assets = table.shape

    @pl.when(step == 0)
    def _():
        for i in range(pieces):
            rows[i * piece : (i + 1) * piece, :] = shock_refs[i][...]

    size = tanh_ref.shape[0]
    shocks = rows[pl.ds(pl.multiple_of(step * size, size), size), :]
    turned_ref[...] = shocks.T
    pnl = jnp.zeros((size, desks), F32)
    for low in range(0, assets, TILE):
        part = slice(low, low + TILE)
        exposure = dot_of(shocks, load_ref[part, :], ((1,), (1,)))
        size_of = jnp.abs(exposure)
        bend = size_of + (jnp.log(1.0 + jnp.exp(-2.0 * size_of)) - LOG2)
        held = asset_ref[1:2, part] * (exposure + asset_ref[0:1, part] * bend)
        tanh_ref[:, part] = jnp.tanh(exposure).astype(BF16)
        bend_ref[:, part] = bend.astype(BF16)
        pnl = pnl + dot_of(held.astype(BF16), table[:, part], ((1,), (1,)))
    pnl_ref[...] = pnl
    row = lax.broadcasted_iota(jnp.int32, (8, desks), 0)
    weigh = jnp.where(row == 0, -1.0, jnp.where(row == 1, asset_ref[3:4, 0:desks], 0.0))
    sums = dot_of(weigh, pnl, ((1,), (1,)), lax.Precision.HIGHEST)
    lines = size // LANES
    for part in range(2):
        for line in range(lines):
            sums_ref[0, part * lines + line : part * lines + line + 1, :] = sums[
                part : part + 1, line * LANES : (line + 1) * LANES
            ]


def forward_call(shocks, place, order, loadings, table, lines, held):
    pieces, piece, factors = len(shocks), *shocks[0].shape
    scenarios = piece * CLASSES
    desks, assets = table.shape
    size = piece
    first = held is None
    base = place
    whole = lambda shape: pl.BlockSpec(shape, lambda i, o: (0, 0))
    out_shape = (
        jax.ShapeDtypeStruct((scenarios, assets), BF16),
        jax.ShapeDtypeStruct((scenarios, assets), BF16),
        jax.ShapeDtypeStruct((scenarios, desks), F32),
        jax.ShapeDtypeStruct((factors, scenarios), BF16),
        jax.ShapeDtypeStruct((CLASSES, 8, LANES), F32),
    )
    out_specs = (
        pl.BlockSpec((size, assets), lambda i, o: (base + i, 0)),
        pl.BlockSpec((size, assets), lambda i, o: (base + i, 0)),
        pl.BlockSpec((size, desks), lambda i, o: (base + i, 0)),
        pl.BlockSpec((factors, size), lambda i, o: (0, base + i)),
        pl.BlockSpec((1, 8, LANES), lambda i, o: (o[place + i], 0, 0)),
    )
    in_specs = [whole((piece, factors))] * pieces + [
        whole((assets, factors)),
        whole((desks, assets)),
        whole((8, assets)),
    ]
    operands = [*shocks, loadings, table, lines]
    aliases = {}
    if not first:
        aliases = {1 + len(operands) + i: i for i in range(5)}
        in_specs += [pl.BlockSpec(memory_space=pl.ANY)] * 5
        operands += list(held)
    return pl.pallas_call(
        lambda *refs: forward_kernel(pieces, first, *refs),
        grid_spec=pltpu.PrefetchScalarGridSpec(
            num_scalar_prefetch=1,
            grid=(pieces,),
            in_specs=in_specs,
            out_specs=out_specs,
            scratch_shapes=[
                pltpu.VMEM((pieces * piece, factors), BF16),
            ],
        ),
        out_shape=out_shape,
        input_output_aliases=aliases,
        compiler_params=pltpu.CompilerParams(
            dimension_semantics=("arbitrary",), vmem_limit_bytes=FORWARD_VMEM
        ),
        cost_estimate=pl.CostEstimate(
            flops=2 * pieces * piece * assets * (factors + desks),
            bytes_accessed=pieces * piece * assets * 4,
            transcendentals=3 * pieces * piece * assets,
        ),
        name=f"forward_{place}",
    )(order, *operands)


def total(x):
    x = jnp.sum(x, axis=0, keepdims=True)
    x = jnp.sum(x, axis=1, keepdims=True)
    return jnp.sum(x, axis=2, keepdims=True)


def tail_of(losses, valued, ranks):
    scenarios = losses.size
    place = (
        lax.broadcasted_iota(jnp.int32, losses.shape, 0) * (losses.shape[1] * LANES)
        + lax.broadcasted_iota(jnp.int32, losses.shape, 1) * LANES
        + lax.broadcasted_iota(jnp.int32, losses.shape, 2)
    )
    offsets = (ranks - CENTER) / BAND
    every = (place.astype(F32) - CENTER) / BAND
    kernel = jnp.exp(-0.5 * offsets * offsets) / total(jnp.exp(-0.5 * every * every))
    quantile = total(kernel * losses)
    average = total(losses) / scenarios
    centred = losses - average
    smoothing = 0.3 * jnp.sqrt(total(centred * centred) / scenarios + 1e-06)
    scores = (losses - quantile) / smoothing
    weights = 1.0 / (1.0 + jnp.exp(-scores))
    weight_total = total(weights)
    objective = -total(weights * valued) / weight_total
    slopes = (-valued - objective) / weight_total * weights * (1.0 - weights)
    grad_quant = -total(slopes) / smoothing
    grad_band = -total(slopes * scores) / smoothing
    grad_loss = (
        slopes / smoothing
        + kernel * grad_quant
        + grad_band * 0.09 * centred / (scenarios * smoothing)
    )
    return (-scenarios * weights / weight_total, -scenarios * grad_loss)


def backward_kernel(order_ref, *refs):
    sums_ref, ranks_ref, tanh_ref, bend_ref, pnl_ref, turned_ref = refs[:6]
    asset_ref = refs[6]
    raw_ref, line_ref, last_ref, scaled, lines, wide, placed, both = refs[7:]
    step = pl.program_id(0)
    factors, scenarios = turned_ref.shape
    desks = pnl_ref.shape[1]
    piece = scenarios // CLASSES
    cuts = piece // LANES

    @pl.when(step == 0)
    def _():
        low = lax.broadcasted_iota(jnp.int32, (1, LANES), 1) < LANES // 2
        for q in range(cuts):
            for j in range(cuts):
                here = ranks_ref[2 * j * cuts + q : 2 * j * cuts + q + 1, :].astype(F32)
                there = ranks_ref[(2 * j + 1) * cuts + q : (2 * j + 1) * cuts + q + 1, :].astype(F32)
                placed[2 * q, j : j + 1, :] = jnp.where(low, here, pltpu.roll(there, LANES // 2, 1))
                placed[2 * q + 1, j : j + 1, :] = jnp.where(
                    low, pltpu.roll(here, LANES // 2, 1), there
                )
        w, g = tail_of(sums_ref[:, 0:cuts, :], sums_ref[:, cuts : 2 * cuts, :], placed[...])
        both[:, 0:cuts, :] = w
        both[:, cuts : 2 * cuts, :] = g
        alloc = jnp.zeros((8, desks), F32)
        sum_w = jnp.zeros((factors, LANES), F32)
        sum_g = jnp.zeros((factors, LANES), F32)
        for i in range(CLASSES):
            kind = order_ref[i]
            rows_w, rows_g = [], []
            for j in range(cuts):
                span = slice(i * piece + j * LANES, i * piece + (j + 1) * LANES)
                turned = turned_ref[:, span].astype(F32)
                row_w = both[kind, j : j + 1, :]
                row_g = both[kind, cuts + j : cuts + j + 1, :]
                by_w = turned * row_w
                by_g = turned * row_g
                sum_w = sum_w + by_w
                sum_g = sum_g + by_g
                scaled[0:factors, span] = by_w.astype(BF16)
                scaled[factors : 2 * factors, span] = by_g.astype(BF16)
                rows_w.append(row_w)
                rows_g.append(row_g)
            row_w = jnp.concatenate(rows_w, axis=1)
            row_g = jnp.concatenate(rows_g, axis=1)
            wide_w = jnp.broadcast_to(row_w, (8, piece))
            wide_g = jnp.broadcast_to(row_g, (8, piece))
            place = lax.broadcasted_iota(jnp.int32, (8, piece), 0)
            value = jnp.where(place < 2, wide_w, wide_g)
            high = value.astype(BF16).astype(F32)
            lines[:, i * piece : (i + 1) * piece] = jnp.where(place % 2 == 0, high, value - high).astype(
                BF16
            )
            alloc = alloc + dot_of(
                wide_w, pnl_ref[i * piece : (i + 1) * piece, :], ((1,), (0,)), lax.Precision.HIGHEST
            )
        wide[:, 0:1] = jnp.sum(sum_w, axis=1, keepdims=True)
        wide[:, 1:2] = jnp.sum(sum_g, axis=1, keepdims=True)
        last_ref[:, 0:desks] = alloc[0:1, :] / scenarios
        last_ref[:, desks : 2 * desks] = jnp.zeros((1, desks), F32)

    part = pl.ds(pl.multiple_of(step * TILE, TILE), TILE)
    conv, held, prices = asset_ref[0:1, part], asset_ref[1:2, part], asset_ref[2:3, part]
    curved = dot_of(scaled[...], tanh_ref[:, part], ((1,), (0,)))
    bent = dot_of(lines[...], bend_ref[:, part], ((1,), (0,)))
    line = held * (prices * (bent[0:1, :] + bent[1:2, :]) + (bent[2:3, :] + bent[3:4, :]))
    raw = (conv * held) * (prices * curved[0:factors, :] + curved[factors:, :]) + held * (
        prices * wide[:, 0:1] + wide[:, 1:2]
    )
    raw_ref[...] = raw.T
    line_ref[...] = line
    squares = jnp.sum(raw * raw, axis=0, keepdims=True) + line * line
    for low in range(0, squares.shape[1], desks):
        last_ref[:, desks : 2 * desks] += squares[:, low : low + desks]


def backward_call(order, sums, ranks, held, lines):
    tanh, bend, pnl, turned = held
    scenarios, assets = tanh.shape
    factors, desks = turned.shape[0], pnl.shape[1]
    whole = lambda *shape: pl.BlockSpec(shape, lambda i, o: (0,) * len(shape))
    line = pl.BlockSpec((1, TILE), lambda i, o: (0, i))
    return pl.pallas_call(
        backward_kernel,
        grid_spec=pltpu.PrefetchScalarGridSpec(
            num_scalar_prefetch=1,
            grid=(assets // TILE,),
            in_specs=[
                whole(*sums.shape),
                whole(*ranks.shape),
                whole(scenarios, assets),
                whole(scenarios, assets),
                whole(scenarios, desks),
                whole(factors, scenarios),
                whole(8, assets),
            ],
            out_specs=(
                pl.BlockSpec((TILE, factors), lambda i, o: (i, 0)),
                line,
                whole(1, 2 * desks),
            ),
            scratch_shapes=[
                pltpu.VMEM((2 * factors, scenarios), BF16),
                pltpu.VMEM((8, scenarios), BF16),
                pltpu.VMEM((factors, 2), F32),
                pltpu.VMEM((CLASSES, sums.shape[1] // 2, LANES), F32),
                pltpu.VMEM(sums.shape, F32),
            ],
        ),
        out_shape=(
            jax.ShapeDtypeStruct((assets, factors), F32),
            jax.ShapeDtypeStruct((1, assets), F32),
            jax.ShapeDtypeStruct((1, 2 * desks), F32),
        ),
        compiler_params=pltpu.CompilerParams(
            dimension_semantics=("arbitrary",), vmem_limit_bytes=BACKWARD_VMEM
        ),
        cost_estimate=pl.CostEstimate(
            flops=4 * scenarios * assets * factors,
            bytes_accessed=scenarios * assets * 4,
            transcendentals=0,
        ),
        name="backward",
    )(order, sums, ranks, tanh, bend, pnl, turned, lines)


def scale_kernel(entries, parts_ref, raw_ref, line_ref, alloc_ref, grad_ref, conv_ref):
    whole = jnp.sum(parts_ref[...], axis=0)
    desks = alloc_ref.shape[1]
    alloc_ref[...] = whole[:, 0:desks]
    squares = jnp.sum(whole[:, desks:], axis=1, keepdims=True)
    factor = lax.rsqrt(squares / entries + 1e-06)
    grad_ref[...] = raw_ref[...] * factor
    conv_ref[...] = line_ref[...] * factor


def scale_call(parts, raw, line, entries):
    desks = parts.shape[2] // 2
    return pl.pallas_call(
        lambda *refs: scale_kernel(entries, *refs),
        out_shape=(
            jax.ShapeDtypeStruct((1, desks), F32),
            jax.ShapeDtypeStruct(raw.shape, F32),
            jax.ShapeDtypeStruct(line.shape, F32),
        ),
        compiler_params=pltpu.CompilerParams(vmem_limit_bytes=SCALE_VMEM),
        name="scale",
    )(parts, raw, line)


def summed_kernel(x_ref, out_ref):
    out_ref[...] = jnp.broadcast_to(jnp.sum(x_ref[...], axis=0, keepdims=True), out_ref.shape)


def summed_copies(x, copies):
    return pl.pallas_call(
        summed_kernel,
        out_shape=jax.ShapeDtypeStruct((copies, *x.shape[1:]), F32),
        compiler_params=pltpu.CompilerParams(vmem_limit_bytes=1 << 20),
        name="summed_copies",
    )(x)


def for_each(x, axis):
    return lax.all_to_all(
        jnp.broadcast_to(x, (lax.axis_size(axis), *x.shape)), axis, 0, 0, tiled=True
    )


def shards(scen_draws, factor_mix, loadings, convexity, holdings, desk_map, ranks, desk_prices):
    chips = FAR * NEAR
    near, core = lax.axis_index("near"), lax.axis_index("core")
    order = ((near + STEPS_Z) % NEAR) * 2 + (core + OTHER) % 2
    up = [(i, (i - 1) % chips) for i in range(chips)]
    down = [(i, (i + 1) % chips) for i in range(chips)]
    swap = lambda x: lax.ppermute(x, "core", [(0, 1), (1, 0)])
    from_up = lambda x: lax.ppermute(x, CHIPS, up)
    from_down = lambda x: lax.ppermute(x, CHIPS, down)

    order, scen_draws = lax.optimization_barrier((order, scen_draws))
    copies, table, lines = prepare_call(
        scen_draws,
        factor_mix,
        desk_map.reshape(1, -1),
        desk_prices.reshape(1, -1),
        convexity.reshape(1, -1),
        holdings.reshape(1, -1),
    )
    own = lax.all_to_all(copies, "far", 0, 0, tiled=True).reshape(-1, copies.shape[2])
    half = own.shape[0] // 2
    forward = lambda shocks, place, held: forward_call(
        shocks, place, order, loadings, table, lines, held
    )
    next_up, next_down = from_up(own), from_down(own)
    own_other = swap(own)
    held = forward([own, own_other], 0, None)
    next_up, next_down, held = lax.optimization_barrier((next_up, next_down, held))
    two_up = from_up(next_up[:half])
    two_down = from_down(next_down[half:])
    up_other, down_other = swap(next_up), swap(next_down)
    held = forward([next_up, next_down, up_other, down_other], 2, held)
    two_up, two_down, held = lax.optimization_barrier((two_up, two_down, held))
    two = jnp.concatenate([two_up, two_down])
    two_other = swap(two)
    held = forward([two], 6, held)
    two_other, held = lax.optimization_barrier((two_other, held))
    held = forward([two_other], 7, held)

    mine = summed_copies(lax.all_to_all(held[4], CLOSE, 0, 0, tiled=True), FAR)
    mine = summed_copies(lax.all_to_all(mine, "far", 0, 0, tiled=True), CLASSES)
    sums = lax.all_to_all(mine, CLOSE, 0, 0, tiled=True)
    placed = ranks.reshape(-1, LANES)
    raw, line, last = backward_call(order, sums, placed, held[:4], lines)
    entries = loadings.shape[0] * lax.axis_size(ASSET) * (loadings.shape[1] + 1)
    alloc, grad, conv = scale_call(for_each(last + swap(last), CHIPS), raw, line, entries)
    return (alloc.reshape(-1), grad, conv.reshape(-1))


def solution(mesh):
    torus = Mesh(
        mesh.devices.reshape(mesh.shape["groups"], FAR, NEAR, 2), ("groups", *ASSET)
    )
    return jax.shard_map(
        shards,
        mesh=torus,
        in_specs=(
            P(GROUPS_ASSET, None),
            P(),
            P(GROUPS_ASSET, None),
            P(GROUPS_ASSET),
            P(GROUPS_ASSET),
            P(GROUPS_ASSET),
            P("groups"),
            P("groups"),
        ),
        out_specs=(P("groups"), P(GROUPS_ASSET, None), P(GROUPS_ASSET)),
        check_vma=False,
    )
```

```python
import math

import jax
import jax.numpy as jnp
import numpy as np
from jax import lax
from jax.experimental import pallas as pl
from jax.experimental.pallas import tpu as pltpu
from jax.sharding import Mesh
from jax.sharding import PartitionSpec as P

BAND = 32
CENTER = 166
FAR = 8
NEAR = 4
CLASSES = NEAR * 2
CHIPS = ("far", "near")
CLOSE = ("near", "core")
ASSET = ("far", "near", "core")
GROUPS_ASSET = ("groups", *ASSET)
LOG2 = math.log(2.0)
F32 = jnp.float32
BF16 = jnp.bfloat16
LANES = 128
TILE = 256
PREPARE_VMEM = 65_900_000
FORWARD_VMEM = 16 << 20
BACKWARD_VMEM = 20 << 20
SCALE_VMEM = 8 << 20
STEPS_Z = np.array([0, 0, 1, 3, 1, 3, 2, 2], np.int32)
OTHER = np.array([0, 1, 0, 0, 1, 1, 0, 1], np.int32)


def dot_of(a, b, dims, precision=None):
    return lax.dot_general(a, b, (dims, ((), ())), precision=precision, preferred_element_type=F32)


def prepare_kernel(*refs):
    given, refs = refs[:6], refs[6:]
    copies_ref, table_ref, asset_ref = refs[:3]
    draws, mix, conv, hold, desk, price, sems = refs[3:]
    moves = [
        pltpu.make_async_copy(source, target, sems.at[i])
        for i, (source, target) in enumerate(
            zip(given, (draws, mix, desk, price, conv, hold))
        )
    ]
    for move in moves:
        move.start()
    for move in moves[:2]:
        move.wait()
    local = dot_of(draws[...], mix[...], ((1,), (0,))).astype(BF16)
    copies_ref[...] = jnp.broadcast_to(local[None], copies_ref.shape)
    for move in moves[2:]:
        move.wait()
    desks, assets = table_ref.shape
    place = lax.broadcasted_iota(jnp.int32, (desks, assets), 0)
    own = jnp.where(place == desk[...], 1.0, 0.0)
    table_ref[...] = own.astype(BF16)
    wide = jnp.broadcast_to(price[...], (8, desks))
    asset_ref[0:1, :] = conv[...]
    asset_ref[1:2, :] = hold[...]
    asset_ref[2:3, :] = dot_of(wide, own, ((1,), (0,)), lax.Precision.HIGHEST)[0:1, :]
    asset_ref[3:4, 0:desks] = price[...]


def prepare_call(scen_draws, factor_mix, desk_map, prices, convexity, holdings):
    assets, desks = desk_map.shape[1], prices.shape[1]
    hbm = pl.BlockSpec(memory_space=pltpu.HBM)
    vmem = pl.BlockSpec(memory_space=pltpu.VMEM)
    row = pltpu.VMEM((1, assets), F32)
    return pl.pallas_call(
        prepare_kernel,
        in_specs=[hbm] * 6,
        out_specs=(vmem,) * 3,
        out_shape=(
            jax.ShapeDtypeStruct((FAR, *scen_draws.shape), BF16),
            jax.ShapeDtypeStruct((desks, assets), BF16),
            jax.ShapeDtypeStruct((8, assets), F32),
        ),
        scratch_shapes=[
            pltpu.VMEM(scen_draws.shape, BF16),
            pltpu.VMEM(factor_mix.shape, BF16),
            row,
            row,
            pltpu.VMEM((1, assets), jnp.int32),
            pltpu.VMEM((1, desks), F32),
            pltpu.SemaphoreType.DMA((6,)),
        ],
        compiler_params=pltpu.CompilerParams(vmem_limit_bytes=PREPARE_VMEM),
        name="prepare",
    )(scen_draws, factor_mix, desk_map, prices, convexity, holdings)


def forward_kernel(pieces, first, order_ref, *refs):
    shock_refs, refs = refs[:pieces], refs[pieces:]
    load_ref, table, asset_ref = refs[:3]
    outs = refs[3:] if first else refs[8:]
    tanh_ref, bend_ref, pnl_ref, turned_ref, sums_ref, rows = outs
    step = pl.program_id(0)
    piece = shock_refs[0].shape[0]
    desks, assets = table.shape

    @pl.when(step == 0)
    def _():
        for i in range(pieces):
            rows[i * piece : (i + 1) * piece, :] = shock_refs[i][...]

    size = tanh_ref.shape[0]
    shocks = rows[pl.ds(pl.multiple_of(step * size, size), size), :]
    turned_ref[...] = shocks.T
    pnl = jnp.zeros((size, desks), F32)
    for low in range(0, assets, TILE):
        part = slice(low, low + TILE)
        exposure = dot_of(shocks, load_ref[part, :], ((1,), (1,)))
        size_of = jnp.abs(exposure)
        bend = size_of + (jnp.log(1.0 + jnp.exp(-2.0 * size_of)) - LOG2)
        held = asset_ref[1:2, part] * (exposure + asset_ref[0:1, part] * bend)
        tanh_ref[:, part] = jnp.tanh(exposure).astype(BF16)
        bend_ref[:, part] = bend.astype(BF16)
        pnl = pnl + dot_of(held.astype(BF16), table[:, part], ((1,), (1,)))
    pnl_ref[...] = pnl
    row = lax.broadcasted_iota(jnp.int32, (8, desks), 0)
    weigh = jnp.where(row == 0, -1.0, jnp.where(row == 1, asset_ref[3:4, 0:desks], 0.0))
    sums = dot_of(weigh, pnl, ((1,), (1,)), lax.Precision.HIGHEST)
    lines = size // LANES
    for part in range(2):
        for line in range(lines):
            sums_ref[0, part * lines + line : part * lines + line + 1, :] = sums[
                part : part + 1, line * LANES : (line + 1) * LANES
            ]


def forward_call(shocks, place, order, loadings, table, lines, held):
    pieces, piece, factors = len(shocks), *shocks[0].shape
    scenarios = piece * CLASSES
    desks, assets = table.shape
    size = piece
    first = held is None
    base = place
    whole = lambda shape: pl.BlockSpec(shape, lambda i, o: (0, 0))
    out_shape = (
        jax.ShapeDtypeStruct((scenarios, assets), BF16),
        jax.ShapeDtypeStruct((scenarios, assets), BF16),
        jax.ShapeDtypeStruct((scenarios, desks), F32),
        jax.ShapeDtypeStruct((factors, scenarios), BF16),
        jax.ShapeDtypeStruct((CLASSES, 8, LANES), F32),
    )
    out_specs = (
        pl.BlockSpec((size, assets), lambda i, o: (base + i, 0)),
        pl.BlockSpec((size, assets), lambda i, o: (base + i, 0)),
        pl.BlockSpec((size, desks), lambda i, o: (base + i, 0)),
        pl.BlockSpec((factors, size), lambda i, o: (0, base + i)),
        pl.BlockSpec((1, 8, LANES), lambda i, o: (o[place + i], 0, 0)),
    )
    in_specs = [whole((piece, factors))] * pieces + [
        whole((assets, factors)),
        whole((desks, assets)),
        whole((8, assets)),
    ]
    operands = [*shocks, loadings, table, lines]
    aliases = {}
    if not first:
        aliases = {1 + len(operands) + i: i for i in range(5)}
        in_specs += [pl.BlockSpec(memory_space=pl.ANY)] * 5
        operands += list(held)
    return pl.pallas_call(
        lambda *refs: forward_kernel(pieces, first, *refs),
        grid_spec=pltpu.PrefetchScalarGridSpec(
            num_scalar_prefetch=1,
            grid=(pieces,),
            in_specs=in_specs,
            out_specs=out_specs,
            scratch_shapes=[
                pltpu.VMEM((pieces * piece, factors), BF16),
            ],
        ),
        out_shape=out_shape,
        input_output_aliases=aliases,
        compiler_params=pltpu.CompilerParams(
            dimension_semantics=("arbitrary",), vmem_limit_bytes=FORWARD_VMEM
        ),
        cost_estimate=pl.CostEstimate(
            flops=2 * pieces * piece * assets * (factors + desks),
            bytes_accessed=pieces * piece * assets * 4,
            transcendentals=3 * pieces * piece * assets,
        ),
        name=f"forward_{place}",
    )(order, *operands)


def total(x):
    x = jnp.sum(x, axis=0, keepdims=True)
    x = jnp.sum(x, axis=1, keepdims=True)
    return jnp.sum(x, axis=2, keepdims=True)


def tail_of(losses, valued, ranks):
    scenarios = losses.size
    place = (
        lax.broadcasted_iota(jnp.int32, losses.shape, 0) * (losses.shape[1] * LANES)
        + lax.broadcasted_iota(jnp.int32, losses.shape, 1) * LANES
        + lax.broadcasted_iota(jnp.int32, losses.shape, 2)
    )
    offsets = (ranks - CENTER) / BAND
    every = (place.astype(F32) - CENTER) / BAND
    kernel = jnp.exp(-0.5 * offsets * offsets) / total(jnp.exp(-0.5 * every * every))
    quantile = total(kernel * losses)
    average = total(losses) / scenarios
    centred = losses - average
    smoothing = 0.3 * jnp.sqrt(total(centred * centred) / scenarios + 1e-06)
    scores = (losses - quantile) / smoothing
    weights = 1.0 / (1.0 + jnp.exp(-scores))
    weight_total = total(weights)
    objective = -total(weights * valued) / weight_total
    slopes = (-valued - objective) / weight_total * weights * (1.0 - weights)
    grad_quant = -total(slopes) / smoothing
    grad_band = -total(slopes * scores) / smoothing
    grad_loss = (
        slopes / smoothing
        + kernel * grad_quant
        + grad_band * 0.09 * centred / (scenarios * smoothing)
    )
    return (-scenarios * weights / weight_total, -scenarios * grad_loss)


def backward_kernel(order_ref, *refs):
    sums_ref, ranks_ref, tanh_ref, bend_ref, pnl_ref, turned_ref = refs[:6]
    asset_ref = refs[6]
    raw_ref, line_ref, last_ref, scaled, lines, wide, placed, both = refs[7:]
    step = pl.program_id(0)
    factors, scenarios = turned_ref.shape
    desks = pnl_ref.shape[1]
    piece = scenarios // CLASSES
    cuts = piece // LANES

    @pl.when(step == 0)
    def _():
        low = lax.broadcasted_iota(jnp.int32, (1, LANES), 1) < LANES // 2
        for q in range(cuts):
            for j in range(cuts):
                here = ranks_ref[2 * j * cuts + q : 2 * j * cuts + q + 1, :].astype(F32)
                there = ranks_ref[(2 * j + 1) * cuts + q : (2 * j + 1) * cuts + q + 1, :].astype(F32)
                placed[2 * q, j : j + 1, :] = jnp.where(low, here, pltpu.roll(there, LANES // 2, 1))
                placed[2 * q + 1, j : j + 1, :] = jnp.where(
                    low, pltpu.roll(here, LANES // 2, 1), there
                )
        w, g = tail_of(sums_ref[:, 0:cuts, :], sums_ref[:, cuts : 2 * cuts, :], placed[...])
        both[:, 0:cuts, :] = w
        both[:, cuts : 2 * cuts, :] = g
        alloc = jnp.zeros((8, desks), F32)
        sum_w = jnp.zeros((factors, LANES), F32)
        sum_g = jnp.zeros((factors, LANES), F32)
        for i in range(CLASSES):
            kind = order_ref[i]
            rows_w, rows_g = [], []
            for j in range(cuts):
                span = slice(i * piece + j * LANES, i * piece + (j + 1) * LANES)
                turned = turned_ref[:, span].astype(F32)
                row_w = both[kind, j : j + 1, :]
                row_g = both[kind, cuts + j : cuts + j + 1, :]
                by_w = turned * row_w
                by_g = turned * row_g
                sum_w = sum_w + by_w
                sum_g = sum_g + by_g
                scaled[0:factors, span] = by_w.astype(BF16)
                scaled[factors : 2 * factors, span] = by_g.astype(BF16)
                rows_w.append(row_w)
                rows_g.append(row_g)
            row_w = jnp.concatenate(rows_w, axis=1)
            row_g = jnp.concatenate(rows_g, axis=1)
            wide_w = jnp.broadcast_to(row_w, (8, piece))
            wide_g = jnp.broadcast_to(row_g, (8, piece))
            place = lax.broadcasted_iota(jnp.int32, (8, piece), 0)
            value = jnp.where(place < 2, wide_w, wide_g)
            high = value.astype(BF16).astype(F32)
            lines[:, i * piece : (i + 1) * piece] = jnp.where(place % 2 == 0, high, value - high).astype(
                BF16
            )
            alloc = alloc + dot_of(
                wide_w, pnl_ref[i * piece : (i + 1) * piece, :], ((1,), (0,)), lax.Precision.HIGHEST
            )
        wide[:, 0:1] = jnp.sum(sum_w, axis=1, keepdims=True)
        wide[:, 1:2] = jnp.sum(sum_g, axis=1, keepdims=True)
        last_ref[:, 0:desks] = alloc[0:1, :] / scenarios
        last_ref[:, desks : 2 * desks] = jnp.zeros((1, desks), F32)

    part = pl.ds(pl.multiple_of(step * TILE, TILE), TILE)
    conv, held, prices = asset_ref[0:1, part], asset_ref[1:2, part], asset_ref[2:3, part]
    curved = dot_of(scaled[...], tanh_ref[:, part], ((1,), (0,)))
    bent = dot_of(lines[...], bend_ref[:, part], ((1,), (0,)))
    line = held * (prices * (bent[0:1, :] + bent[1:2, :]) + (bent[2:3, :] + bent[3:4, :]))
    raw = (conv * held) * (prices * curved[0:factors, :] + curved[factors:, :]) + held * (
        prices * wide[:, 0:1] + wide[:, 1:2]
    )
    raw_ref[...] = raw.T
    line_ref[...] = line
    squares = jnp.sum(raw * raw, axis=0, keepdims=True) + line * line
    for low in range(0, squares.shape[1], desks):
        last_ref[:, desks : 2 * desks] += squares[:, low : low + desks]


def backward_call(order, sums, ranks, held, lines):
    tanh, bend, pnl, turned = held
    scenarios, assets = tanh.shape
    factors, desks = turned.shape[0], pnl.shape[1]
    whole = lambda *shape: pl.BlockSpec(shape, lambda i, o: (0,) * len(shape))
    line = pl.BlockSpec((1, TILE), lambda i, o: (0, i))
    return pl.pallas_call(
        backward_kernel,
        grid_spec=pltpu.PrefetchScalarGridSpec(
            num_scalar_prefetch=1,
            grid=(assets // TILE,),
            in_specs=[
                whole(*sums.shape),
                whole(*ranks.shape),
                whole(scenarios, assets),
                whole(scenarios, assets),
                whole(scenarios, desks),
                whole(factors, scenarios),
                whole(8, assets),
            ],
            out_specs=(
                pl.BlockSpec((TILE, factors), lambda i, o: (i, 0)),
                line,
                whole(1, 2 * desks),
            ),
            scratch_shapes=[
                pltpu.VMEM((2 * factors, scenarios), BF16),
                pltpu.VMEM((8, scenarios), BF16),
                pltpu.VMEM((factors, 2), F32),
                pltpu.VMEM((CLASSES, sums.shape[1] // 2, LANES), F32),
                pltpu.VMEM(sums.shape, F32),
            ],
        ),
        out_shape=(
            jax.ShapeDtypeStruct((assets, factors), F32),
            jax.ShapeDtypeStruct((1, assets), F32),
            jax.ShapeDtypeStruct((1, 2 * desks), F32),
        ),
        compiler_params=pltpu.CompilerParams(
            dimension_semantics=("arbitrary",), vmem_limit_bytes=BACKWARD_VMEM
        ),
        cost_estimate=pl.CostEstimate(
            flops=4 * scenarios * assets * factors,
            bytes_accessed=scenarios * assets * 4,
            transcendentals=0,
        ),
        name="backward",
    )(order, sums, ranks, tanh, bend, pnl, turned, lines)


def scale_kernel(entries, parts_ref, raw_ref, line_ref, alloc_ref, grad_ref, conv_ref):
    whole = jnp.sum(parts_ref[...], axis=0)
    desks = alloc_ref.shape[1]
    alloc_ref[...] = whole[:, 0:desks]
    squares = jnp.sum(whole[:, desks:], axis=1, keepdims=True)
    factor = lax.rsqrt(squares / entries + 1e-06)
    grad_ref[...] = raw_ref[...] * factor
    conv_ref[...] = line_ref[...] * factor


def scale_call(parts, raw, line, entries):
    desks = parts.shape[2] // 2
    return pl.pallas_call(
        lambda *refs: scale_kernel(entries, *refs),
        out_shape=(
            jax.ShapeDtypeStruct((1, desks), F32),
            jax.ShapeDtypeStruct(raw.shape, F32),
            jax.ShapeDtypeStruct(line.shape, F32),
        ),
        compiler_params=pltpu.CompilerParams(vmem_limit_bytes=SCALE_VMEM),
        name="scale",
    )(parts, raw, line)


def summed_kernel(x_ref, out_ref):
    out_ref[...] = jnp.broadcast_to(jnp.sum(x_ref[...], axis=0, keepdims=True), out_ref.shape)


def summed_copies(x, copies):
    return pl.pallas_call(
        summed_kernel,
        out_shape=jax.ShapeDtypeStruct((copies, *x.shape[1:]), F32),
        compiler_params=pltpu.CompilerParams(vmem_limit_bytes=1 << 20),
        name="summed_copies",
    )(x)


def for_each(x, axis):
    return lax.all_to_all(
        jnp.broadcast_to(x, (lax.axis_size(axis), *x.shape)), axis, 0, 0, tiled=True
    )


def shards(scen_draws, factor_mix, loadings, convexity, holdings, desk_map, ranks, desk_prices):
    chips = FAR * NEAR
    near, core = lax.axis_index("near"), lax.axis_index("core")
    up = [(i, (i - 1) % chips) for i in range(chips)]
    down = [(i, (i + 1) % chips) for i in range(chips)]
    swap = lambda x: lax.ppermute(x, "core", [(0, 1), (1, 0)])
    from_up = lambda x: lax.ppermute(x, CHIPS, up)
    from_down = lambda x: lax.ppermute(x, CHIPS, down)

    copies, table, lines = prepare_call(
        scen_draws,
        factor_mix,
        desk_map.reshape(1, -1),
        desk_prices.reshape(1, -1),
        convexity.reshape(1, -1),
        holdings.reshape(1, -1),
    )
    own = lax.all_to_all(copies, "far", 0, 0, tiled=True).reshape(-1, copies.shape[2])
    own, near, core = lax.optimization_barrier((own, near, core))
    order = ((near + STEPS_Z) % NEAR) * 2 + (core + OTHER) % 2
    half = own.shape[0] // 2
    forward = lambda shocks, place, held: forward_call(
        shocks, place, order, loadings, table, lines, held
    )
    next_up, next_down = from_up(own), from_down(own)
    own_other = swap(own)
    held = forward([own, own_other], 0, None)
    next_up, next_down, held = lax.optimization_barrier((next_up, next_down, held))
    two_up = from_up(next_up[:half])
    two_down = from_down(next_down[half:])
    up_other, down_other = swap(next_up), swap(next_down)
    held = forward([next_up, next_down, up_other, down_other], 2, held)
    two_up, two_down, held = lax.optimization_barrier((two_up, two_down, held))
    two = jnp.concatenate([two_up, two_down])
    two_other = swap(two)
    held = forward([two], 6, held)
    two_other, held = lax.optimization_barrier((two_other, held))
    held = forward([two_other], 7, held)

    mine = summed_copies(lax.all_to_all(held[4], CLOSE, 0, 0, tiled=True), FAR)
    mine = summed_copies(lax.all_to_all(mine, "far", 0, 0, tiled=True), CLASSES)
    sums = lax.all_to_all(mine, CLOSE, 0, 0, tiled=True)
    placed = ranks.reshape(-1, LANES)
    raw, line, last = backward_call(order, sums, placed, held[:4], lines)
    entries = loadings.shape[0] * lax.axis_size(ASSET) * (loadings.shape[1] + 1)
    alloc, grad, conv = scale_call(for_each(last + swap(last), CHIPS), raw, line, entries)
    return (alloc.reshape(-1), grad, conv.reshape(-1))


def solution(mesh):
    torus = Mesh(
        mesh.devices.reshape(mesh.shape["groups"], FAR, NEAR, 2), ("groups", *ASSET)
    )
    return jax.shard_map(
        shards,
        mesh=torus,
        in_specs=(
            P(GROUPS_ASSET, None),
            P(),
            P(GROUPS_ASSET, None),
            P(GROUPS_ASSET),
            P(GROUPS_ASSET),
            P(GROUPS_ASSET),
            P("groups"),
            P("groups"),
        ),
        out_specs=(P("groups"), P(GROUPS_ASSET, None), P(GROUPS_ASSET)),
        check_vma=False,
    )
```
